256 devices in a mesh: grp: 4 (over z_lo), mem: 64 (over x, z_hi, y, core).
Axes of the slice: x: 4, y: 4, z: 8 (z_hi: 2, z_lo: 4; z = z_hi * 4 + z_lo), core: 2. Of those that a mesh axis runs over, the one named last changes fastest.
Arguments:
- embeddings: bfloat16 [262144, 4096], P(('grp', 'mem')), may hold values from -6 to 6
- local_picks: int32 [4, 512], P('grp', 'mem'), may hold values from 0 to 1023
- second_picks: int32 [4, 16], P('grp'), may hold values from 0 to 511
- final_picks: int32 [16], replicated, may hold values from 0 to 63
Outputs:
- gain_table: float32 [64, 512], P('grp', 'mem')
- final_cover: float32 [262144], P(('grp', 'mem'))
The draws below stay inside these ranges and needn't reach their ends.
Inputs may be any that keep to these rules, and one draw needn't show every extreme that they name: `local_picks`: entry (g, m * 8 + k) names a row among the 1024 points of device m of group g; repeats may occur. `second_picks`: candidate indices of the group, in greedy order; repeats may occur. `final_picks`: index g * 16 + t names group g's second-round pick t; repeats may occur.
All inputs are finite; a program needn't handle non-finite values.
Results may differ from the reference program's by a relative error of at most 0.0003.
Values may be sent and summed in bfloat16 or wider, within the bound.
A program may use at most 64 MiB of HBM per device.

```python
import jax
import jax.numpy as jnp
from jax import lax

D = 4096
P_DEV = 1024
K1 = 8
K2 = 16
K3 = 16
CANDS = 512
UNION = 64
POINTS = 262144
N_GRP = 4
N_MEM = 64


def plant(result, own_key, low, top_value):
    spot = [jax.random.randint(jax.random.fold_in(own_key, axis), (), 0, length) for axis, length in enumerate(result.shape)]
    widest = result.shape.index(max(result.shape))
    beside = spot[:widest] + [(spot[widest] + 1) % result.shape[widest]] + spot[widest + 1:]
    return result.at[tuple(spot)].set(low).at[tuple(beside)].set(top_value)


def steps_of(key, shape, pieces, low, largest):
    level, own = 1.0, jax.random.fold_in(key, 6)
    for position, blocks in pieces:
        heights = jnp.exp(jax.random.uniform(jax.random.fold_in(own, position), (blocks,), jnp.float32, low / len(pieces), largest / len(pieces)))
        level = level * jnp.repeat(heights, shape[position] // blocks).reshape([-1 if axis == position else 1 for axis in range(len(shape))])
    return level


def normal_values(stream_key, shape, spread, most, cuts=(), held_as=jnp.bfloat16):
    drawn = spread * jax.random.normal(stream_key, shape, jnp.float32)
    if cuts:
        drawn = drawn * steps_of(stream_key, shape, cuts, -0.22, 0.18)
    return jnp.clip(drawn, -most, most).astype(held_as)


def setup_inputs(seed: int = 0) -> dict:
    key_list = jax.random.split(jax.random.key(seed), 5)
    embeddings = normal_values(key_list[0], (POINTS, D), 1.0, 6.0, ((0, 256),))
    local_picks = plant(jax.random.randint(key_list[1], (N_GRP, CANDS), 0, P_DEV), jax.random.fold_in(key_list[1], 1), 0, P_DEV - 1).astype(jnp.int32)
    second_picks = plant(jax.random.randint(key_list[2], (N_GRP, K2), 0, CANDS), jax.random.fold_in(key_list[2], 1), 0, CANDS - 1).astype(jnp.int32)
    final_picks = plant(jax.random.randint(key_list[3], (K3,), 0, UNION), jax.random.fold_in(key_list[3], 1), 0, UNION - 1).astype(jnp.int32)
    return {"embeddings": embeddings, "local_picks": local_picks, "second_picks": second_picks, "final_picks": final_picks}


def reference(embeddings, local_picks, second_picks, final_picks):
    scaling = float(D) ** -0.5
    grouped = embeddings.reshape(N_GRP, N_MEM, P_DEV, D)
    pick_rows = local_picks.reshape(N_GRP, N_MEM, K1).astype(jnp.int32)
    candidates = jax.vmap(jax.vmap(lambda points, chosen: jnp.take(points, chosen, axis=0)))(grouped, pick_rows)
    candidates = candidates.reshape(N_GRP, CANDS, D)
    winners = jax.vmap(lambda cands, chosen: jnp.take(cands, chosen, axis=0))(candidates, second_picks.astype(jnp.int32))
    winners = winners.reshape(UNION, D)
    final_rows = jnp.take(winners, final_picks.astype(jnp.int32), axis=0)

    def group_gains(inputs):
        cand_group, points_group, second_group = inputs

        def device_step(running, device_inputs):
            point_rows, member = device_inputs
            similar_map = jnp.dot(point_rows, cand_group.T, preferred_element_type=jnp.float32) * scaling
            own_block = lax.dynamic_slice_in_dim(similar_map, member * K1, K1, 1)
            coverage = jnp.max(own_block, axis=1)
            chosen_cols = jnp.take(similar_map, second_group, axis=1)

            def greedy_step(cover_now, column):
                partial_value = jnp.sum(jnp.maximum(similar_map - cover_now[:, None], 0.0), axis=0)
                return jnp.maximum(cover_now, column), partial_value

            _, partials = lax.scan(greedy_step, coverage, chosen_cols.T)
            return running + partials, None

        start_sum = jnp.zeros((K2, CANDS), jnp.float32)
        running, _ = lax.scan(device_step, start_sum, (points_group, jnp.arange(N_MEM, dtype=jnp.int32)))
        return running / P_DEV

    gain_table = lax.map(group_gains, (candidates, grouped, second_picks.astype(jnp.int32)))
    gain_table = gain_table.reshape(N_GRP * K2, CANDS)

    def device_cover(point_rows):
        return jnp.max(jnp.dot(point_rows, final_rows.T, preferred_element_type=jnp.float32) * scaling, axis=1)

    final_cover = lax.map(device_cover, embeddings.reshape(N_GRP * N_MEM, P_DEV, D)).reshape(POINTS)
    return gain_table, final_cover
```

```python
import functools

import jax
import jax.numpy as jnp
from jax import lax
from jax.experimental import pallas as pl
from jax.experimental.pallas import tpu as pltpu
from jax.sharding import PartitionSpec as P

MESH = pl.DeviceIdType.MESH
F32 = jnp.float32
BF16 = jnp.bfloat16

D = 4096
P_DEV = 1024
K1 = 8
ROUNDS = 16
FINALS = 16
N_MEM = 64
N_GRP = 4
SIDE = 4
J = 4
KC = D // J
X_PARTS = 8
NT = 256
HALF = J // 2
ORDER = ["l0", "l1", "l2", "l3", "a0", "a1", "a2", "a3", "l4", "l5", "b0", "b1", "l6", "l7"]
ORDER += ["a4", "a5", "b2", "b3", "c0", "c1", "a6", "a7", "c2", "c3", "b4", "b5", "b6", "b7"]
ORDER += ["c4", "c5", "m0", "m1", "c6", "c7", "m2", "m3"]


def kernel(
    local_ref, second_ref, final_ref, x_hbm, gain_ref, cover_ref,
    xs, cand, sim, cov, cov_sum, gains, arrived, f_rows, f_send, f_recv, f_all,
    load_sem, z_send, z_recv, light_send, light_recv, heavy_send, heavy_recv,
    d2d_send, d2d_recv, a2a_send, a2a_recv, fs_send, fs_recv, fd_send, fd_recv,
):
    g = lax.axis_index("grp")
    m = lax.axis_index("mem")
    c = m % 2
    y = (m // 2) % SIDE
    z = (m // 8) % 2
    x = m // 16
    turn = 1 - 2 * c

    def device(xx, zz, yy, cc):
        return (g, ((xx * 2 + zz) * SIDE + yy) * 2 + cc)

    def around(v, step):
        return (v + step + SIDE) % SIDE

    rows8 = P_DEV // 8 // X_PARTS
    loads = [
        pltpu.make_async_copy(
            x_hbm.at[pl.ds(i * rows8, rows8)], xs.at[pl.ds(i * rows8, rows8)], load_sem.at[i]
        )
        for i in range(X_PARTS)
    ]
    for copy in loads:
        copy.start()

    barrier = pltpu.get_barrier_semaphore()
    greeted = [device(around(x, s), z, y, c) for s in (1, 2, 3)]
    greeted += [device(x, z, around(y, s), c) for s in (1, 2, 3)]
    greeted += [device(x, 1 - z, y, c), device(x, z, y, 1 - c)]
    greeted += [((g + s) % N_GRP, m) for s in (1, 2, 3)]
    for other in greeted:
        pl.semaphore_signal(barrier, inc=1, device_id=other, device_id_type=MESH)

    for copy in loads:
        copy.wait()

    sub8 = lax.broadcasted_iota(jnp.int32, (8, D), 0)
    own = jnp.zeros((8, D), F32)
    for k in range(K1):
        r = local_ref[0, k]
        tile = xs[r // 8].astype(F32)
        row = jnp.sum(jnp.where(sub8 == r % 8, tile, 0.0), axis=0, keepdims=True)
        own = jnp.where(sub8 == k, row, own)
    own = own.astype(BF16)
    for j in range(J):
        cand[j, x, z, y, c] = own[:, j * KC : (j + 1) * KC]

    pl.semaphore_wait(barrier, len(greeted))

    def remote(src, send, recv, to):
        return pltpu.make_async_remote_copy(
            src_ref=src, dst_ref=src, send_sem=send, recv_sem=recv, device_id=to, device_id_type=MESH
        )

    def z_copy(j):
        src = cand.at[j, x, z, y, c]
        return remote(src, z_send.at[j], z_recv.at[j], device(x, 1 - z, y, c))

    def plane(i):
        return z if i < J else 1 - z

    def x_first(i):
        return i % 2 == 0

    def light(i, s):
        src = cand.at[i % J, x, plane(i), y, c]
        to = device(around(x, s), z, y, c) if x_first(i) else device(x, z, around(y, s), c)
        return remote(src, light_send.at[i, s - 1], light_recv.at[i, s - 1], to)

    def row_of(i, b, cc):
        if x_first(i):
            return cand.at[i % J, :, plane(i), b, cc]
        return cand.at[i % J, b, plane(i), :, cc]

    def place(i):
        return y if x_first(i) else x

    def beside(i, s):
        if x_first(i):
            return device(x, z, around(y, s), c)
        return device(around(x, s), z, y, c)

    def heavy(i, slot):
        b = place(i)
        if slot == 2:
            src, to = row_of(i, around(b, -turn), c), beside(i, turn)
        else:
            src, to = row_of(i, b, c), beside(i, 1 if slot == 0 else -1)
        return remote(src, heavy_send.at[i, slot], heavy_recv.at[i, slot], to)

    def across(i, step):
        src = row_of(i, around(place(i), step), c)
        return remote(src, d2d_send.at[i, step], d2d_recv.at[i, step], device(x, z, y, 1 - c))

    def stage_l(i):
        if i >= J:
            z_copy(i - J).wait_recv()
        for s in (1, 3, 2):
            light(i, s).start()

    def stage_a(i):
        for s in (1, 2, 3):
            light(i, s).wait_recv()
        heavy(i, 0).start()
        heavy(i, 1).start()
        across(i, 0).start()

    def stage_b(i):
        heavy(i, 0).wait_recv()
        heavy(i, 1).wait_recv()
        heavy(i, 2).start()
        across(i, 1).start()
        across(i, 3).start()

    def stage_c(i):
        heavy(i, 2).wait_recv()
        across(i, 2).start()

    def stage_m(j):
        for i in (j, j + J):
            for step in range(SIDE):
                across(i, step).wait_recv()

        def tile(n, carry):
            at = pl.multiple_of(n * (NT // 8), NT // 8)
            lhs = cand[j].reshape(N_MEM * K1, KC)
            rhs = xs[pl.ds(at, NT // 8), :, j * KC : (j + 1) * KC].reshape(NT, KC)
            part = lax.dot_general(
                lhs, rhs, (((1,), (1,)), ((), ())), preferred_element_type=F32
            ).reshape(N_MEM, K1, NT)
            cols = pl.ds(pl.multiple_of(n * NT, NT), NT)
            if j == 0:
                sim[:, :, cols] = part
            else:
                sim[:, :, cols] += part
            return carry

        lax.fori_loop(0, P_DEV // NT, tile, 0)

    for j in range(J):
        z_copy(j).start()
    stages = {"l": stage_l, "a": stage_a, "b": stage_b, "c": stage_c, "m": stage_m}
    for word in ORDER:
        stages[word[0]](int(word[1:]))

    sub_h = lax.broadcasted_iota(jnp.int32, (8, KC), 0)

    def pick_final(q, carry):
        f = final_ref[q]
        chosen = second_ref[0, f % ROUNDS]
        owner = chosen // K1
        keep = jnp.where(f // ROUNDS == g, chosen % K1, 8)
        for h in range(HALF):
            tile = cand[c * HALF + h, owner // 16, (owner // 8) % 2, (owner // 2) % SIDE, owner % 2]
            row = jnp.sum(jnp.where(sub_h == keep, tile.astype(F32), 0.0), axis=0, keepdims=True)
            f_rows[h, pl.ds(q, 1), :] = row
        return carry

    lax.fori_loop(0, FINALS, pick_final, 0)
    f_send[...] = f_rows[...].astype(BF16)

    cover = jnp.max(sim[m], axis=0, keepdims=True)
    sub_p = lax.broadcasted_iota(jnp.int32, (8, P_DEV), 0)
    for t in range(ROUNDS):
        wide = jnp.broadcast_to(cover, (8, P_DEV))
        cov[t] = wide
        total = wide[:, 0:128]
        for u in range(1, P_DEV // 128):
            total = total + wide[:, u * 128 : (u + 1) * 128]
        cov_sum[t] = total
        chosen = second_ref[0, t]
        tile = jnp.where(sub_p == chosen % K1, sim[chosen // K1], -jnp.inf)
        cover = jnp.maximum(cover, jnp.max(tile, axis=0, keepdims=True))

    def final_copy(s):
        return pltpu.make_async_remote_copy(
            src_ref=f_send, dst_ref=f_recv.at[s - 1], send_sem=fs_send.at[s - 1],
            recv_sem=fs_recv.at[s - 1], device_id=((g + s) % N_GRP, m), device_id_type=MESH,
        )

    for s in (1, 2, 3):
        final_copy(s).start()

    lane = lax.broadcasted_iota(jnp.int32, (8, 128), 1)
    sub = lax.broadcasted_iota(jnp.int32, (8, 128), 0)

    def member_at(e):
        zz = jnp.where(e < 32, 1 - z, z)
        xx = (x + (e // 8) % 4) % SIDE
        yy = (y + (e // 2) % 4) % SIDE
        cc = (c + e + 1) % 2
        return ((xx * 2 + zz) * SIDE + yy) * 2 + cc

    def result_copy(to):
        return pltpu.make_async_remote_copy(
            src_ref=gains.at[to], dst_ref=arrived.at[m], send_sem=a2a_send, recv_sem=a2a_recv,
            device_id=(g, to), device_id_type=MESH,
        )

    def send_pair(i):
        for e in (2 * i, 2 * i + 1):
            to = member_at(e)

            @pl.when(to != m)
            def _():
                result_copy(to).start()

    def gain_pair(i, carry):
        @pl.when(i > 0)
        def _():
            send_pair(i - 1)

        a, b = member_at(2 * i), member_at(2 * i + 1)
        out_a = jnp.zeros((8, 128), F32)
        out_b = jnp.zeros((8, 128), F32)
        tile_a, tile_b = sim[a], sim[b]
        for t in range(ROUNDS):
            sum_a = sum_b = None
            for u in range(P_DEV // 128):
                now = cov[t, :, u * 128 : (u + 1) * 128]
                over_a = jnp.maximum(tile_a[:, u * 128 : (u + 1) * 128], now)
                over_b = jnp.maximum(tile_b[:, u * 128 : (u + 1) * 128], now)
                sum_a = over_a if u == 0 else sum_a + over_a
                sum_b = over_b if u == 0 else sum_b + over_b
            sum_a = jnp.sum(sum_a - cov_sum[t], axis=1, keepdims=True)
            sum_b = jnp.sum(sum_b - cov_sum[t], axis=1, keepdims=True)
            out_a = jnp.where(lane % ROUNDS == t, sum_a, out_a)
            out_b = jnp.where(lane % ROUNDS == t, sum_b, out_b)
        for to, out in ((a, out_a), (b, out_b)):
            gains[to] = jnp.sum(jnp.where(lane // ROUNDS == sub, out, 0.0), axis=0, keepdims=True)
        return carry

    lax.fori_loop(0, N_MEM // 2, gain_pair, 0)
    arrived[m] = gains[m]
    send_pair(N_MEM // 2 - 1)

    for s in (1, 2, 3):
        final_copy(s).wait_recv()
    rows = f_send[...].astype(F32)
    for s in range(3):
        rows = rows + f_recv[s].astype(F32)
    f_all[pl.ds(c * HALF, HALF)] = rows.astype(BF16)
    half_copy = remote(f_all.at[pl.ds(c * HALF, HALF)], fd_send, fd_recv, device(x, z, y, 1 - c))
    half_copy.start()
    half_copy.wait_recv()

    def final_tile(n, carry):
        at = pl.multiple_of(n * (NT // 8), NT // 8)
        part = jnp.zeros((NT, FINALS), F32)
        for j in range(J):
            lhs = xs[pl.ds(at, NT // 8), :, j * KC : (j + 1) * KC].reshape(NT, KC)
            part = part + lax.dot_general(
                lhs, f_all[j], (((1,), (1,)), ((), ())), preferred_element_type=F32
            )
        best = jnp.max(part.T, axis=0, keepdims=True) * (D**-0.5)
        cover_ref[:, pl.ds(pl.multiple_of(n * NT, NT), NT)] = best
        return carry

    lax.fori_loop(0, P_DEV // NT, final_tile, 0)

    several = pl.ds(0, N_MEM - 1)
    pltpu.make_async_copy(arrived.at[several], arrived.at[several], a2a_recv).wait()
    gain_ref[...] = jnp.sum(arrived[...], axis=0) * (D**-0.5 / P_DEV)

    pltpu.make_async_copy(gains.at[several], gains.at[several], a2a_send).wait()
    half_copy.wait_send()
    for s in (1, 2, 3):
        final_copy(s).wait_send()
    for j in range(J):
        z_copy(j).wait_send()
    for i in range(2 * J):
        for s in (1, 2, 3):
            light(i, s).wait_send()
        for slot in range(3):
            heavy(i, slot).wait_send()
        for step in range(SIDE):
            across(i, step).wait_send()


def per_device(embeddings, local_picks, second_picks, final_picks):
    smem = pl.BlockSpec(memory_space=pltpu.SMEM)
    vmem = pl.BlockSpec(memory_space=pltpu.VMEM)
    dma = pltpu.SemaphoreType.DMA
    gain, cover = pl.pallas_call(
        kernel,
        out_shape=(
            jax.ShapeDtypeStruct((1, 128), F32),
            jax.ShapeDtypeStruct((1, P_DEV), F32),
        ),
        in_specs=[smem, smem, smem, pl.BlockSpec(memory_space=pl.ANY)],
        out_specs=(vmem, vmem),
        scratch_shapes=[
            pltpu.VMEM((P_DEV // 8, 8, D), BF16),
            pltpu.VMEM((J, SIDE, 2, SIDE, 2, K1, KC), BF16),
            pltpu.VMEM((N_MEM, K1, P_DEV), F32),
            pltpu.VMEM((ROUNDS, 8, P_DEV), F32),
            pltpu.VMEM((ROUNDS, 8, 128), F32),
            pltpu.VMEM((N_MEM, 1, 128), F32),
            pltpu.VMEM((N_MEM, 1, 128), F32),
            pltpu.VMEM((HALF, FINALS, KC), F32),
            pltpu.VMEM((HALF, FINALS, KC), BF16),
            pltpu.VMEM((3, HALF, FINALS, KC), BF16),
            pltpu.VMEM((J, FINALS, KC), BF16),
            dma((X_PARTS,)),
            dma((J,)),
            dma((J,)),
            dma((2 * J, 3)),
            dma((2 * J, 3)),
            dma((2 * J, 3)),
            dma((2 * J, 3)),
            dma((2 * J, SIDE)),
            dma((2 * J, SIDE)),
            dma,
            dma,
            dma((3,)),
            dma((3,)),
            dma,
            dma,
        ],
        compiler_params=pltpu.CompilerParams(collective_id=0, has_side_effects=True),
        name="coreset",
    )(local_picks, second_picks, final_picks, embeddings.reshape(P_DEV // 8, 8, D))
    return gain.reshape(K1, ROUNDS).T, cover.reshape(P_DEV)


def solution(mesh):
    placed = (P(("grp", "mem"), None), P("grp", "mem"), P("grp", None), P())
    return jax.shard_map(
        per_device,
        mesh=mesh,
        in_specs=placed,
        out_specs=(P("grp", "mem"), P(("grp", "mem"))),
        check_vma=False,
    )
```
